256 devices in a mesh: row: 8 (over y, x_lo), col: 32 (over x_hi, z, core).
Axes of the slice: x: 4 (x_hi: 2, x_lo: 2; x = x_hi * 2 + x_lo), y: 4, z: 8, core: 2. Of those that a mesh axis runs over, the one named last changes fastest.
Arguments:
- inverse_state: float32 [4, 2048, 1, 8192], P(None, 'row', None, 'col')
- row_seeds: int32 [2, 4, 2048], P(None, None, 'row'), may hold values from 0 to 31
- col_seeds: int32 [2, 1, 8192], P(None, None, 'col'), may hold values from 0 to 31
Outputs:
- inverse: float32 [4, 2048, 1, 8192], P(None, 'row', None, 'col')
The draws below stay inside these ranges and needn't reach their ends.
All inputs are finite; a program needn't handle non-finite values.
Results may differ from the reference program's by a relative error of at most 0.0002.
Values sent between devices are 32-bit elements; how exact they have to be, the bound alone decides.
No kernel may reach another device: no remote copies, remote signals or barrier semaphores. Data moves between devices by JAX's collectives and lax.ppermute only.
A program may use at most 64 MiB of HBM per device.

```python
import jax
import jax.numpy as jnp
from jax import lax

N = 8192
NB = 256
STEPS = 2
N_ROW = 8
N_COL = 32


def orthogonal_block(key):
    gauss = jax.random.normal(key, (NB, NB), jnp.float32)
    basis, upper = jnp.linalg.qr(gauss)
    return basis


def draw_inverse_state(key, part):
    key_base = jax.random.fold_in(key, 11)
    base = jax.random.normal(key_base, (N, N), jnp.float32)
    low_end = 2.0 * jnp.sqrt(jnp.float32(NB))
    high_end = 4.0 * low_end
    for step in range(STEPS):
        key_sing = jax.random.fold_in(key, 100 + step)
        key_left = jax.random.fold_in(key, 200 + step)
        key_right = jax.random.fold_in(key, 300 + step)
        singular = jnp.exp(jax.random.uniform(key_sing, (NB,), jnp.float32, 0.0, 1.0) * jnp.log(high_end / low_end)) * low_end
        left_basis = orthogonal_block(key_left)
        right_basis = orthogonal_block(key_right)
        pivot = jnp.dot(left_basis * singular[None, :], right_basis.T, precision=lax.Precision.HIGHEST, preferred_element_type=jnp.float32)
        start = N - (STEPS - step) * NB
        base = base.at[start:start + NB, start:start + NB].set(pivot)
    return base.reshape(N // (N_ROW * NB), N_ROW * NB, N // (N_COL * NB), N_COL * NB)


def place_ends(values, stream_key, low, high):
    dims = values.shape
    index_at = [jax.random.randint(jax.random.fold_in(stream_key, axis), (), 0, dims[axis]) for axis in range(len(dims))]
    values = values.at[tuple(index_at)].set(low)
    longest = dims.index(max(dims))
    index_at[longest] = (index_at[longest] + 1) % dims[longest]
    return values.at[tuple(index_at)].set(high)


def setup_inputs(seed: int = 0) -> dict:
    keys = jax.random.split(jax.random.key(seed), 4)
    return {
        "inverse_state": draw_inverse_state(jax.random.fold_in(keys[3], 71), 0),
        "row_seeds": place_ends(jax.random.randint(keys[1], (2, N // (N_ROW * NB), N_ROW * NB), 0, 32), jax.random.fold_in(keys[1], 1), 0, 31).astype(jnp.int32),
        "col_seeds": place_ends(jax.random.randint(keys[2], (2, N // (N_COL * NB), N_COL * NB), 0, 32), jax.random.fold_in(keys[2], 1), 0, 31).astype(jnp.int32),
    }


root_half = 0.7071067811865476

def level_apply(matrix, scales, groups):
    count = matrix.shape[0]
    half = count // (2 * groups)
    shaped = matrix.reshape(groups, 2, half, matrix.shape[1])
    factor = scales.reshape(groups, 2, half, 1)
    upper = factor[:, 0] * shaped[:, 0]
    lower = factor[:, 1] * shaped[:, 1]
    return (jnp.stack([upper + lower, upper - lower], axis=1) * root_half).reshape(matrix.shape)

def butterfly(matrix, seeds):
    scales = (2.0 * seeds.reshape(2, N).astype(jnp.float32) - 31.0) / 16.0
    return level_apply(level_apply(matrix, scales[0], 1), scales[1], 2)

def reference(inverse_state, row_seeds, col_seeds):
    matrix = inverse_state.reshape(N, N)
    identity = jnp.eye(NB, dtype=jnp.float32)
    for step in range(STEPS):
        start = N - (STEPS - step) * NB
        stop = start + NB
        pivot = matrix[start:stop, start:stop]
        shifted = matrix.at[:, start:stop].set(0.0)
        shifted = shifted.at[start:stop, start:stop].set(identity)
        right_part = jnp.linalg.solve(pivot, shifted[start:stop])
        left_part = matrix[:, start:stop].at[start:stop].set(pivot - identity)
        matrix = shifted - jnp.dot(left_part.astype(jnp.float32), right_part.astype(jnp.float32), precision=lax.Precision.HIGHEST, preferred_element_type=jnp.float32)
    rows_done = butterfly(matrix, row_seeds)
    result = butterfly(rows_done.T, col_seeds).T
    return result.reshape(inverse_state.shape)
```

```python
import jax
import jax.numpy as jnp
from jax import lax
from jax.sharding import PartitionSpec as P

STEPS = 2
root_half = 0.7071067811865476
HIGHEST = lax.Precision.HIGHEST


def seed_values(seeds):
    return (2.0 * seeds.astype(jnp.float32) - 31.0) / 16.0


def dot(a, b):
    return jnp.dot(a, b, precision=HIGHEST, preferred_element_type=jnp.float32)


def halves_level(parts, scales, groups):
    count = parts.shape[0]
    half = count // (2 * groups)
    shaped = parts.reshape((groups, 2, half) + parts.shape[1:])
    factor = scales.reshape((groups, 2, half) + scales.shape[1:])
    upper = factor[:, 0] * shaped[:, 0]
    lower = factor[:, 1] * shaped[:, 1]
    return (jnp.stack([upper + lower, upper - lower], axis=1) * root_half).reshape(parts.shape)


def butterfly(parts, scales):
    return halves_level(halves_level(parts, scales[0], 1), scales[1], 2)


def inverse_block(pivot):
    gram = dot(pivot.T, pivot)
    factor = jnp.linalg.cholesky(gram)
    middle = lax.linalg.triangular_solve(factor, pivot.T, left_side=True, lower=True)
    return lax.linalg.triangular_solve(factor, middle, left_side=True, lower=True, transpose_a=True)


def pivot_inverse(m00, m01, m10, m11):
    first = inverse_block(m00)
    left = dot(m10, first)
    right = dot(first, m01)
    second = inverse_block(m11 - dot(left, m01))
    upper = -dot(right, second)
    lower = -dot(second, left)
    corner = first - dot(upper, left)
    return jnp.concatenate(
        [jnp.concatenate([corner, upper], 1), jnp.concatenate([lower, second], 1)], 0
    )


def shift_pairs(count, move, chosen):
    return [(i, move(i)) for i in range(count) if chosen(i)]


def per_device(inverse_state, row_seeds, col_seeds):
    blocks, block = inverse_state.shape[:2]
    rows, cols = lax.axis_size("row"), lax.axis_size("col")
    row, col = lax.axis_index("row"), lax.axis_index("col")
    strip = block // cols
    state = inverse_state.reshape(blocks, block, block)
    last = blocks - 1
    low, high = cols - 2, cols - 1
    same_core = [[2 * i + core for i in range(cols // 2)] for core in range(2)]
    identity = jnp.eye(block, dtype=jnp.float32)
    eye_strip = lax.dynamic_slice_in_dim(identity, col * strip, strip, 0)
    odd = col % 2 == 1

    def exchange(parts):
        return lax.all_to_all(parts, "col", 0, 0)

    def spread(part):
        copies = jnp.broadcast_to(part, (cols // 2,) + part.shape)
        near = lax.all_to_all(copies, "col", 0, 0, axis_index_groups=same_core)
        far = lax.ppermute(near, "col", [(i, i ^ 1) for i in range(cols)])
        return jnp.stack([jnp.where(odd, far, near), jnp.where(odd, near, far)], axis=1)

    tail = exchange(state[last].reshape(cols, strip, block))
    head = exchange(
        state[:last].reshape(last, cols, strip, block).transpose(1, 0, 2, 3)
    )
    own_seeds = seed_values(col_seeds.reshape(2, block))
    all_seeds = exchange(jnp.broadcast_to(own_seeds, (cols,) + own_seeds.shape))
    col_scales = all_seeds.transpose(1, 0, 2)

    pivot_part = jnp.stack([tail[low], tail[high]])
    from_rows = lax.all_to_all(
        jnp.broadcast_to(pivot_part, (rows,) + pivot_part.shape), "row", 0, 0
    )
    pivot_all = spread(from_rows[rows - 2 :])
    pivot_all = pivot_all.transpose(2, 3, 0, 1, 4, 5).reshape(2, 2, block, block)

    is_low, is_high = row == rows - 2, row == rows - 1
    tail_fixed = tail.at[low].set(jnp.where(is_low, eye_strip, 0.0))
    tail_fixed = tail_fixed.at[high].set(jnp.where(is_high, eye_strip, 0.0))
    tail_back = exchange(butterfly(tail_fixed, col_scales[:, :, None, :])).reshape(block, block)
    head_fixed = head.at[low:].set(0.0)
    head_back = exchange(butterfly(head_fixed, col_scales[:, :, None, None, :]))
    head_back = head_back.transpose(1, 0, 2, 3).reshape(last, block, block)

    def row_fan(step):
        return lax.ppermute(
            tail_back, "row", [(i, (i + 2 * step) % rows) for i in (rows - 2, rows - 1)]
        )

    near = row_fan(1) + row_fan(2) + row_fan(3)
    near = jnp.where(row >= rows - 2, tail_back, near)
    far = lax.ppermute(near, "row", [(i, i ^ 1) for i in range(rows)])
    odd_row = row % 2 == 1
    pivot_rows = jnp.concatenate(
        [jnp.where(odd_row, far, near), jnp.where(odd_row, near, far)], 0
    )

    row_scales = seed_values(row_seeds)
    own_scales = lax.dynamic_slice_in_dim(row_scales, col * strip, strip, 2)[..., None, :, None]
    left = jnp.concatenate(
        [
            head[low:].transpose(1, 0, 2, 3),
            jnp.stack(
                [
                    tail[low] - jnp.where(is_low, eye_strip, 0.0),
                    tail[high] - jnp.where(is_high, eye_strip, 0.0),
                ]
            )[None],
        ],
        0,
    )
    left = spread(butterfly(left, own_scales))
    left = left.transpose(2, 0, 1, 4, 3, 5).reshape(blocks * block, 2 * block)

    inverse = pivot_inverse(pivot_all[0, 0], pivot_all[0, 1], pivot_all[1, 0], pivot_all[1, 1])
    right = dot(inverse, pivot_rows)
    moved = butterfly(
        jnp.concatenate([head_back, tail_back[None]], 0), row_scales[..., None]
    )
    result = moved.reshape(blocks * block, block) - dot(left, right)
    return result.reshape(inverse_state.shape)


def solution(mesh):
    placed = (P(None, "row", None, "col"), P(None, None, "row"), P(None, None, "col"))
    return jax.shard_map(
        per_device,
        mesh=mesh,
        in_specs=placed,
        out_specs=P(None, "row", None, "col"),
        check_vma=False,
    )
```

```python
import jax
import jax.numpy as jnp
from jax import lax
from jax.experimental import pallas as pl
from jax.experimental.pallas import tpu as pltpu
from jax.sharding import PartitionSpec as P

LIMIT = 64
root_half = 0.7071067811865476
HIGHEST = lax.Precision.HIGHEST


def seed_values(seeds):
    return (2.0 * seeds.astype(jnp.float32) - 31.0) / 16.0


def dot(a, b):
    return jnp.dot(a, b, precision=HIGHEST, preferred_element_type=jnp.float32)


def halves_level(parts, scales, groups):
    count = parts.shape[0]
    half = count // (2 * groups)
    shaped = parts.reshape((groups, 2, half) + parts.shape[1:])
    factor = scales.reshape((groups, 2, half) + scales.shape[1:])
    upper = factor[:, 0] * shaped[:, 0]
    lower = factor[:, 1] * shaped[:, 1]
    return (jnp.stack([upper + lower, upper - lower], axis=1) * root_half).reshape(parts.shape)


def butterfly(parts, scales):
    return halves_level(halves_level(parts, scales[0], 1), scales[1], 2)


def kdot(a, b, dims=(((1,), (0,)), ((), ()))):
    return lax.dot_general(a, b, dims, precision=HIGHEST, preferred_element_type=jnp.float32)


def invert_into(p_ref, x_ref, e_ref):
    size = p_ref.shape[0]
    p = p_ref[...]
    top = jnp.max(jnp.abs(p))
    scale = 1.0 / top
    p = p * scale
    p_ref[...] = p
    gram = kdot(p, p, (((1,), (1,)), ((), ())))
    bound = jnp.max(jnp.sum(jnp.abs(gram), axis=0, keepdims=True))
    x_ref[...] = p.T * (1.9 / bound)

    def step():
        row = lax.broadcasted_iota(jnp.int32, (size, size), 0)
        column = lax.broadcasted_iota(jnp.int32, (size, size), 1)
        e = jnp.where(row == column, 1.0, 0.0) - kdot(p_ref[...], x_ref[...])
        e_ref[...] = e
        x_ref[...] += kdot(x_ref[...], e_ref[...])
        return jnp.sum(e * e)

    def unfinished(carry):
        count, error = carry
        return (count < LIMIT) & jnp.logical_not(error < 1e-7)

    def again(carry):
        return carry[0] + 1, step()

    lax.while_loop(unfinished, again, (0, jnp.float32(1.0)))
    x_ref[...] = x_ref[...] * scale


def first_kernel(odd_ref, near_ref, far_ref, first_ref, left_ref, right_ref, schur_ref, p_ref, e_ref):
    odd = odd_ref[0] == 1

    def part(i, j):
        near, far = near_ref[:, i, j], far_ref[:, i, j]
        even_part = jnp.where(odd, far, near)
        odd_part = jnp.where(odd, near, far)
        block = jnp.stack([even_part, odd_part], axis=1)
        return block.reshape(p_ref.shape)

    p_ref[...] = part(0, 0)
    invert_into(p_ref, first_ref, e_ref)
    left_ref[...] = kdot(part(1, 0), first_ref[...])
    p_ref[...] = part(0, 1)
    right_ref[...] = kdot(first_ref[...], p_ref[...])
    schur_ref[...] = part(1, 1) - kdot(left_ref[...], p_ref[...])


def second_kernel(schur_ref, first_ref, left_ref, right_ref, rows_ref, out_ref, p_ref, x_ref, e_ref):
    p_ref[...] = schur_ref[...]
    invert_into(p_ref, x_ref, e_ref)
    e_ref[...] = rows_ref[1] - kdot(left_ref[...], rows_ref[0])
    out_ref[1] = kdot(x_ref[...], e_ref[...])
    out_ref[0] = kdot(first_ref[...], rows_ref[0]) - kdot(right_ref[...], out_ref[1])


def call(kernel, out_shape, scratch, flops, *args):
    smem = [pl.BlockSpec(memory_space=pltpu.SMEM)] if args[0].dtype == jnp.int32 else []
    rest = len(args) - len(smem)
    return pl.pallas_call(
        kernel,
        out_shape=out_shape,
        in_specs=smem + [pl.BlockSpec(memory_space=pltpu.VMEM)] * rest,
        out_specs=jax.tree.map(lambda _: pl.BlockSpec(memory_space=pltpu.VMEM), out_shape),
        scratch_shapes=scratch,
        cost_estimate=pl.CostEstimate(flops=flops, bytes_accessed=1 << 20, transcendentals=0),
    )(*args)


def per_device(inverse_state, row_seeds, col_seeds):
    blocks, block = inverse_state.shape[:2]
    rows, cols = lax.axis_size("row"), lax.axis_size("col")
    row, col = lax.axis_index("row"), lax.axis_index("col")
    strip = block // cols
    state = inverse_state.reshape(blocks, block, block)
    last = blocks - 1
    low, high = cols - 2, cols - 1
    same_core = [[2 * i + core for i in range(cols // 2)] for core in range(2)]
    identity = jnp.eye(block, dtype=jnp.float32)
    eye_strip = lax.dynamic_slice_in_dim(identity, col * strip, strip, 0)
    odd = col % 2 == 1

    def exchange(parts):
        return lax.all_to_all(parts, "col", 0, 0)

    def spread(part):
        copies = jnp.broadcast_to(part, (cols // 2,) + part.shape)
        near = lax.all_to_all(copies, "col", 0, 0, axis_index_groups=same_core)
        far = lax.ppermute(near, "col", [(i, i ^ 1) for i in range(cols)])
        return near, far

    half = block // 2
    own_seeds = seed_values(col_seeds.reshape(2 * 2, half))
    own_seeds = jnp.pad(own_seeds, [(0, strip - 4), (0, 0)])
    packed = jnp.concatenate(
        [
            state[last].reshape(cols, strip, 2, half).transpose(0, 2, 1, 3),
            jnp.broadcast_to(own_seeds, (cols, 1, strip, half)),
        ],
        1,
    )
    packed = exchange(packed)
    tail = packed[:, :2].transpose(0, 2, 1, 3).reshape(cols, strip, block)
    col_scales = packed[:, 2, :4].reshape(cols, 2, block).transpose(1, 0, 2)
    head = exchange(
        state[:last].reshape(last, cols, strip, block).transpose(1, 0, 2, 3)
    )
    pivot_part = jnp.stack([tail[low], tail[high]])
    from_rows = lax.all_to_all(
        jnp.broadcast_to(pivot_part, (rows,) + pivot_part.shape), "row", 0, 0
    )
    pivot_near, pivot_far = spread(from_rows[rows - 2 :])

    is_low, is_high = row == rows - 2, row == rows - 1
    tail_fixed = tail.at[low].set(jnp.where(is_low, eye_strip, 0.0))
    tail_fixed = tail_fixed.at[high].set(jnp.where(is_high, eye_strip, 0.0))
    tail_back = exchange(butterfly(tail_fixed, col_scales[:, :, None, :])).reshape(block, block)
    head_fixed = head.at[low:].set(0.0)
    head_back = exchange(butterfly(head_fixed, col_scales[:, :, None, None, :]))
    head_back = head_back.transpose(1, 0, 2, 3).reshape(last, block, block)

    def row_fan(step):
        return lax.ppermute(
            tail_back, "row", [(i, (i + 2 * step) % rows) for i in (rows - 2, rows - 1)]
        )

    near = row_fan(1) + row_fan(2) + row_fan(3)
    near = jnp.where(row >= rows - 2, tail_back, near)
    far = lax.ppermute(near, "row", [(i, i ^ 1) for i in range(rows)])
    odd_row = row % 2 == 1
    pivot_rows = jnp.stack([jnp.where(odd_row, far, near), jnp.where(odd_row, near, far)])

    row_scales = seed_values(row_seeds)
    own_scales = lax.dynamic_slice_in_dim(row_scales, col * strip, strip, 2)[..., None, :, None]
    left = jnp.concatenate(
        [
            head[low:].transpose(1, 0, 2, 3),
            jnp.stack(
                [
                    tail[low] - jnp.where(is_low, eye_strip, 0.0),
                    tail[high] - jnp.where(is_high, eye_strip, 0.0),
                ]
            )[None],
        ],
        0,
    )
    left_near, left_far = spread(butterfly(left, own_scales))
    left = jnp.stack(
        [jnp.where(odd, left_far, left_near), jnp.where(odd, left_near, left_far)], axis=1
    )
    left = left.transpose(2, 0, 1, 4, 3, 5).reshape(blocks * block, 2 * block)

    matrix = jax.ShapeDtypeStruct((block, block), jnp.float32)
    buffer = pltpu.VMEM((block, block), jnp.float32)
    work = 2 * block**3
    odd_core = (col % 2).astype(jnp.int32).reshape(1)
    first, side, over, schur = call(
        first_kernel, [matrix] * 4, [buffer] * 2, 160 * work, odd_core, pivot_near, pivot_far
    )
    right = call(
        second_kernel,
        jax.ShapeDtypeStruct((2, block, block), jnp.float32),
        [buffer] * 3,
        160 * work,
        schur,
        first,
        side,
        over,
        pivot_rows,
    ).reshape(2 * block, block)
    moved = butterfly(
        jnp.concatenate([head_back, tail_back[None]], 0), row_scales[..., None]
    )
    result = moved.reshape(blocks * block, block) - dot(left, right)
    return result.reshape(inverse_state.shape)


def solution(mesh):
    placed = (P(None, "row", None, "col"), P(None, None, "row"), P(None, None, "col"))
    return jax.shard_map(
        per_device,
        mesh=mesh,
        in_specs=placed,
        out_specs=P(None, "row", None, "col"),
        check_vma=False,
    )
```

```python
import jax
import jax.numpy as jnp
from jax import lax
from jax.experimental import pallas as pl
from jax.experimental.pallas import tpu as pltpu
from jax.sharding import PartitionSpec as P


LIMIT = 64
WARM = 8
root_half = 0.7071067811865476
HIGHEST = lax.Precision.HIGHEST


def seed_values(seeds):
    return (2.0 * seeds.astype(jnp.float32) - 31.0) / 16.0


def halves_level(parts, scales, groups):
    count = parts.shape[0]
    half = count // (2 * groups)
    shaped = parts.reshape((groups, 2, half) + parts.shape[1:])
    factor = scales.reshape((groups, 2, half) + scales.shape[1:])
    upper = factor[:, 0] * shaped[:, 0]
    lower = factor[:, 1] * shaped[:, 1]
    return (jnp.stack([upper + lower, upper - lower], axis=1) * root_half).reshape(parts.shape)


def butterfly(parts, scales):
    return halves_level(halves_level(parts, scales[0], 1), scales[1], 2)


def kdot(a, b, dims=(((1,), (0,)), ((), ())), precision=HIGHEST):
    return lax.dot_general(a, b, dims, precision=precision, preferred_element_type=jnp.float32)


def invert_into(p_ref, x_ref, e_ref):
    size = p_ref.shape[0]
    scale = 1.0 / jnp.max(jnp.abs(p_ref[...]))
    p_ref[...] = p_ref[...] * scale
    gram = kdot(p_ref[...], p_ref[...], (((1,), (1,)), ((), ())))
    factor = 1.9 / jnp.max(jnp.sum(jnp.abs(gram), axis=0, keepdims=True))

    def start():
        x_ref[...] = p_ref[...].T * factor

    def residual(precision):
        row = lax.broadcasted_iota(jnp.int32, (size, size), 0)
        column = lax.broadcasted_iota(jnp.int32, (size, size), 1)
        product = kdot(p_ref[...], x_ref[...], precision=precision)
        e_ref[...] = jnp.where(row == column, 1.0, 0.0) - product

    def advance(precision):
        x_ref[...] += kdot(x_ref[...], e_ref[...], precision=precision)

    def exact_error():
        residual(HIGHEST)
        e = e_ref[...]
        return jnp.sum(e * e)

    start()

    @pl.loop(0, WARM)
    def _(_):
        residual(lax.Precision.DEFAULT)
        advance(lax.Precision.DEFAULT)

    error = exact_error()
    failed = jnp.logical_not(error < 0.5)

    @pl.when(failed)
    def _():
        start()
        residual(HIGHEST)

    def unfinished(carry):
        count, error = carry
        return (count < LIMIT) & jnp.logical_not(error < 1e-7)

    def again(carry):
        advance(HIGHEST)
        return carry[0] + 1, exact_error()

    lax.while_loop(unfinished, again, (0, jnp.where(failed, 1.0, error)))
    advance(HIGHEST)
    x_ref[...] = x_ref[...] * scale


def first_kernel(odd_ref, near_ref, far_ref, first_ref, left_ref, right_ref, schur_ref, p_ref, e_ref):
    odd = odd_ref[0] == 1

    def part(i, j):
        near, far = near_ref[:, i], far_ref[:, i]
        return jnp.where(odd == (j == 1), near, far).reshape(p_ref.shape)

    p_ref[...] = part(0, 0)
    invert_into(p_ref, first_ref, e_ref)
    left_ref[...] = kdot(part(1, 0), first_ref[...])
    p_ref[...] = part(0, 1)
    right_ref[...] = kdot(first_ref[...], p_ref[...])
    schur_ref[...] = part(1, 1) - kdot(left_ref[...], p_ref[...])


def second_kernel(schur_ref, first_ref, left_ref, right_ref, rows_ref, out_ref, p_ref, x_ref, e_ref):
    p_ref[...] = schur_ref[...]
    invert_into(p_ref, x_ref, e_ref)
    e_ref[...] = rows_ref[1] - kdot(left_ref[...], rows_ref[0])
    out_ref[1] = kdot(x_ref[...], e_ref[...])
    out_ref[0] = kdot(first_ref[...], rows_ref[0]) - kdot(right_ref[...], out_ref[1])


def last_kernel(place_ref, base_ref, own_ref, across_ref, twin_ref, other_ref, rows_ref, out_ref):
    odd, half = place_ref[0] == 1, place_ref[1]
    count, blocks, strip, size = own_ref.shape
    tall = count * strip
    for a in range(blocks):
        for side, (same, swapped) in enumerate([(own_ref, twin_ref), (across_ref, other_ref)]):
            one, two = same[:, a].reshape(tall, size), swapped[:, a].reshape(tall, size)
            update = kdot(jnp.where(odd, two, one), rows_ref[0])
            update += kdot(jnp.where(odd, one, two), rows_ref[1])
            top = (half if side == 0 else 1 - half) * tall
            value = base_ref[a, pl.ds(pl.multiple_of(top, tall), tall), :] - update
            for lane in range(size // 128):
                at = pl.ds((a * size + top) * (size // 128) + lane, tall, stride=size // 128)
                out_ref[at, :] = value[:, lane * 128 : (lane + 1) * 128]


def call(kernel, out_shape, scratch, flops, *args):
    smem = [pl.BlockSpec(memory_space=pltpu.SMEM)] if args[0].dtype == jnp.int32 else []
    rest = len(args) - len(smem)
    return pl.pallas_call(
        kernel,
        out_shape=out_shape,
        in_specs=smem + [pl.BlockSpec(memory_space=pltpu.VMEM)] * rest,
        out_specs=jax.tree.map(lambda _: pl.BlockSpec(memory_space=pltpu.VMEM), out_shape),
        scratch_shapes=scratch,
        cost_estimate=pl.CostEstimate(flops=flops, bytes_accessed=1 << 20, transcendentals=0),
    )(*args)


def after(value, *earlier):
    return lax.optimization_barrier((value, *earlier))[0]


def per_device(inverse_state, row_seeds, col_seeds):
    blocks, block = inverse_state.shape[:2]
    rows, cols = lax.axis_size("row"), lax.axis_size("col")
    row, col = lax.axis_index("row"), lax.axis_index("col")
    half, ring, last = cols // 2, cols // 4, blocks - 1
    side, place, core = col // half, col % half // 2, col % 2
    rings = [
        [s * half + p * 2 + c for p in range(ring)] for s in range(2) for c in range(2)
    ]
    state = inverse_state.reshape(blocks, block, block)
    identity = jnp.eye(block, dtype=jnp.float32)
    pivot_col = col >= cols - 2
    diagonal = (col - cols == row - rows) & pivot_col
    row_scales = seed_values(row_seeds)[..., None]
    col_scales = seed_values(col_seeds).reshape(2, 1, block)
    smem = jnp.stack([core, side]).astype(jnp.int32)

    def send(value, pairs, axis="col"):
        return lax.ppermute(value, axis, pairs)

    def flip(value, bit):
        return send(value, [(i, i ^ bit) for i in range(cols)])

    def exchange(parts, axis, groups=None):
        return lax.all_to_all(parts, axis, 0, 0, axis_index_groups=groups)

    def spread(part, count, axis, groups=None):
        return exchange(jnp.broadcast_to(part, (count,) + part.shape), axis, groups)

    def joined(top, own, partner):
        return jnp.where(top, own + partner, partner - own)

    span_one, span_two = half, half // 2
    top_one, top_two = col // span_one % 2 == 0, col // span_two % 2 == 0

    tail = state[last]
    strips = exchange(tail.reshape(rows, block // rows, block), "row")[rows - 2 :]
    crossed = send(strips, [(i, i - half) for i in (cols - 2, cols - 1)])
    both = jnp.where(place == ring - 1, jnp.where(side == 1, strips, crossed), 0.0)

    left = jnp.where(
        diagonal,
        jnp.concatenate([state[:last], (tail - identity)[None]], 0),
        state,
    )
    left = butterfly(left, row_scales)
    tall = block // 2
    crossed = send(left[:, :tall], [(i, i - half) for i in (cols - 2, cols - 1)])
    own_half = jnp.where(side == 1, left[:, tall:], after(crossed, both))

    def hops(step):
        sources = range(2 * step - 1, ring, 2 * step)
        return [(group[p], group[p - step]) for group in rings for p in sources]

    steps = [ring >> (i + 1) for i in range(ring.bit_length() - 1)]

    ready = [both]
    for step in steps:
        ready.append(ready[-1] + send(ready[-1], hops(step)))
    strips = ready[-1]

    piece = own_half
    for i, step in enumerate(steps):
        wide = piece.shape[1] // 2
        moved = after(send(piece[:, :wide], hops(step)), ready[i + 1])
        piece = jnp.where(place % (2 * step) == 2 * step - 1, piece[:, wide:], moved)

    cleared = jnp.where(pivot_col, jnp.where(diagonal, identity, 0.0), tail) * col_scales[0]
    tail_one = joined(top_one, cleared, flip(cleared, span_one)) * root_half
    tail_one = tail_one * col_scales[1]
    partner = after(flip(tail_one, span_two), strips)
    tail_moved = joined(top_two, tail_one, partner) * root_half

    def row_fan(step):
        pairs = [(i, (i + 2 * step) % rows) for i in (rows - 2, rows - 1)]
        return send(tail_moved, pairs, "row")

    near = row_fan(1) + row_fan(2) + row_fan(3)
    near = jnp.where(row >= rows - 2, tail_moved, near)
    far = send(near, [(i, i ^ 1) for i in range(rows)], "row")
    odd_row = row % 2 == 1
    pivot_rows = jnp.stack([jnp.where(odd_row, far, near), jnp.where(odd_row, near, far)])

    pivot_near = spread(strips, rows, "row")
    pivot_near = after(pivot_near, piece, near)
    pivot_far = flip(pivot_near, 1)
    left_own = spread(after(piece, pivot_near), ring, "col", rings)

    second = col_scales[1]
    second_one = flip(second, span_one)
    near_pair = jnp.stack([second, second_one])
    far_pair = flip(near_pair, span_two)
    head = jnp.where(pivot_col, 0.0, state[:last]) * col_scales[0]
    head_far = after(flip(head, span_two), pivot_near)
    head_own = joined(top_two, near_pair[0] * head, far_pair[0] * head_far)
    head_sent = joined(top_two, near_pair[1] * head, far_pair[1] * head_far)
    head_partner = flip(head_sent, span_one)

    matrix = jax.ShapeDtypeStruct((block, block), jnp.float32)
    buffer = pltpu.VMEM((block, block), jnp.float32)
    work = 2 * block**3
    first, below, over, schur = call(
        first_kernel, [matrix] * 4, [buffer] * 2, 160 * work, smem, pivot_near, pivot_far
    )
    left_own = after(left_own, first)
    left_across = flip(left_own, span_one)
    left_twin = flip(left_own, 1)
    right = call(
        second_kernel,
        jax.ShapeDtypeStruct((2, block, block), jnp.float32),
        [buffer] * 3,
        160 * work,
        schur,
        first,
        below,
        over,
        pivot_rows,
    )
    left_across, head_partner = after(left_across, right), after(head_partner, right)
    left_other = flip(left_across, 1)
    head_moved = joined(top_one, head_own, head_partner) * (root_half * root_half)
    moved = butterfly(jnp.concatenate([head_moved, tail_moved[None]], 0), row_scales)
    result = call(
        last_kernel,
        jax.ShapeDtypeStruct((blocks * block * block // 128, 128), jnp.float32),
        [],
        6 * 8 * work,
        smem,
        moved,
        left_own,
        left_across,
        left_twin,
        left_other,
        right,
    )
    return result.reshape(inverse_state.shape)


def solution(mesh):
    placed = (P(None, "row", None, "col"), P(None, None, "row"), P(None, None, "col"))

    return jax.shard_map(
        per_device,
        mesh=mesh,
        in_specs=placed,
        out_specs=P(None, "row", None, "col"),
        check_vma=False,
    )
```

```python
import jax
import jax.numpy as jnp
from jax import lax
from jax.experimental import pallas as pl
from jax.experimental.pallas import tpu as pltpu
from jax.sharding import PartitionSpec as P


LIMIT = 64
WARM = 8
root_half = 0.7071067811865476
HIGHEST = lax.Precision.HIGHEST


def seed_values(seeds):
    return (2.0 * seeds.astype(jnp.float32) - 31.0) / 16.0


def halves_level(parts, scales, groups):
    count = parts.shape[0]
    half = count // (2 * groups)
    shaped = parts.reshape((groups, 2, half) + parts.shape[1:])
    factor = scales.reshape((groups, 2, half) + scales.shape[1:])
    upper = factor[:, 0] * shaped[:, 0]
    lower = factor[:, 1] * shaped[:, 1]
    return (jnp.stack([upper + lower, upper - lower], axis=1) * root_half).reshape(parts.shape)


def butterfly(parts, scales):
    return halves_level(halves_level(parts, scales[0], 1), scales[1], 2)


def kdot(a, b, dims=(((1,), (0,)), ((), ())), precision=HIGHEST):
    return lax.dot_general(a, b, dims, precision=precision, preferred_element_type=jnp.float32)


def invert_into(p_ref, x_ref, e_ref):
    size = p_ref.shape[0]
    scale = 1.0 / jnp.max(jnp.abs(p_ref[...]))
    p_ref[...] = p_ref[...] * scale
    gram = kdot(p_ref[...], p_ref[...], (((1,), (1,)), ((), ())))
    factor = 1.9 / jnp.max(jnp.sum(jnp.abs(gram), axis=0, keepdims=True))

    def start():
        x_ref[...] = p_ref[...].T * factor

    def residual(precision):
        row = lax.broadcasted_iota(jnp.int32, (size, size), 0)
        column = lax.broadcasted_iota(jnp.int32, (size, size), 1)
        product = kdot(p_ref[...], x_ref[...], precision=precision)
        e_ref[...] = jnp.where(row == column, 1.0, 0.0) - product

    def advance(precision):
        x_ref[...] += kdot(x_ref[...], e_ref[...], precision=precision)

    def exact_error():
        residual(HIGHEST)
        e = e_ref[...]
        return jnp.sum(e * e)

    start()

    @pl.loop(0, WARM)
    def _(_):
        residual(lax.Precision.DEFAULT)
        advance(lax.Precision.DEFAULT)

    error = exact_error()
    failed = jnp.logical_not(error < 0.5)

    @pl.when(failed)
    def _():
        start()
        residual(HIGHEST)

    def unfinished(carry):
        count, error = carry
        return (count < LIMIT) & jnp.logical_not(error < 1e-7)

    def again(carry):
        advance(HIGHEST)
        return carry[0] + 1, exact_error()

    lax.while_loop(unfinished, again, (0, jnp.where(failed, 1.0, error)))
    advance(HIGHEST)
    x_ref[...] = x_ref[...] * scale


def first_kernel(odd_ref, near_ref, far_ref, first_ref, left_ref, right_ref, schur_ref, p_ref, e_ref):
    odd = odd_ref[0] == 1
    tall = p_ref.shape[0] // near_ref.shape[0]

    def part(i, j):
        at = pl.ds(i * tall, tall)
        near, far = near_ref[:, at], far_ref[:, at]
        return jnp.where(odd == (j == 1), near, far).reshape(p_ref.shape)

    p_ref[...] = part(0, 0)
    invert_into(p_ref, first_ref, e_ref)
    left_ref[...] = kdot(part(1, 0), first_ref[...])
    p_ref[...] = part(0, 1)
    right_ref[...] = kdot(first_ref[...], p_ref[...])
    schur_ref[...] = part(1, 1) - kdot(left_ref[...], p_ref[...])


def second_kernel(schur_ref, first_ref, left_ref, right_ref, rows_ref, out_ref, p_ref, x_ref, e_ref):
    p_ref[...] = schur_ref[...]
    invert_into(p_ref, x_ref, e_ref)
    e_ref[...] = rows_ref[1] - kdot(left_ref[...], rows_ref[0])
    out_ref[1] = kdot(x_ref[...], e_ref[...])
    out_ref[0] = kdot(first_ref[...], rows_ref[0]) - kdot(right_ref[...], out_ref[1])


def last_kernel(place_ref, base_ref, own_ref, across_ref, twin_ref, other_ref, rows_ref, out_ref):
    odd, lower = place_ref[0] == 1, place_ref[1] == 1
    blocks, size = base_ref.shape[:2]
    parts = size // 128
    strip = size // (2 * own_ref.shape[0])
    skip = own_ref.shape[1] - blocks * strip

    def joined(one_ref, two_ref, a):
        one = one_ref[:, skip + a * strip : skip + (a + 1) * strip]
        two = two_ref[:, a * strip : (a + 1) * strip]
        both = jnp.stack([jnp.where(lower, two, one), jnp.where(lower, one, two)], axis=1)
        return both.reshape(size, size)

    for a in range(blocks):
        same, swapped = joined(own_ref, across_ref, a), joined(twin_ref, other_ref, a)
        update = kdot(jnp.where(odd, swapped, same), rows_ref[0])
        update += kdot(jnp.where(odd, same, swapped), rows_ref[1])
        value = base_ref[a] - update
        for lane in range(parts):
            at = pl.ds(a * size * parts + lane, size, stride=parts)
            out_ref[at, :] = value[:, lane * 128 : (lane + 1) * 128]


def call(kernel, out_shape, scratch, flops, *args):
    smem = [pl.BlockSpec(memory_space=pltpu.SMEM)] if args[0].dtype == jnp.int32 else []
    rest = len(args) - len(smem)
    return pl.pallas_call(
        kernel,
        out_shape=out_shape,
        in_specs=smem + [pl.BlockSpec(memory_space=pltpu.VMEM)] * rest,
        out_specs=jax.tree.map(lambda _: pl.BlockSpec(memory_space=pltpu.VMEM), out_shape),
        scratch_shapes=scratch,
        cost_estimate=pl.CostEstimate(flops=flops, bytes_accessed=1 << 20, transcendentals=0),
    )(*args)


def after(value, *earlier):
    return lax.optimization_barrier((value, *earlier))[0]


def per_device(inverse_state, row_seeds, col_seeds):
    blocks, block = inverse_state.shape[:2]
    rows, cols = lax.axis_size("row"), lax.axis_size("col")
    row, col = lax.axis_index("row"), lax.axis_index("col")
    half, ring, last = cols // 2, cols // 4, blocks - 1
    side, place, core = col // half, col % half // 2, col % 2
    rings = [
        [s * half + p * 2 + c for p in range(ring)] for s in range(2) for c in range(2)
    ]
    state = inverse_state.reshape(blocks, block, block)
    identity = jnp.eye(block, dtype=jnp.float32)
    pivot_col = col >= cols - 2
    diagonal = (col - cols == row - rows) & pivot_col
    row_scales = seed_values(row_seeds)[..., None]
    col_scales = seed_values(col_seeds).reshape(2, 1, block)
    smem = jnp.stack([core, side]).astype(jnp.int32)

    def send(value, pairs, axis="col"):
        return lax.ppermute(value, axis, pairs)

    def flip(value, bit):
        return send(value, [(i, i ^ bit) for i in range(cols)])

    def exchange(parts, axis, groups=None):
        return lax.all_to_all(parts, axis, 0, 0, axis_index_groups=groups)

    def spread(part, count, axis, groups=None):
        return exchange(jnp.broadcast_to(part, (count,) + part.shape), axis, groups)

    def joined(top, own, partner):
        return jnp.where(top, own + partner, partner - own)

    span_one, span_two = half, half // 2
    top_one, top_two = col // span_one % 2 == 0, col // span_two % 2 == 0

    tail = state[last]
    tall = block // ring
    strips = state.reshape(blocks, ring, tall, block).transpose(1, 0, 2, 3)
    strips = exchange(strips, "col", rings)[ring - 1]
    crossing = [(i + half, i) for i in range(half)]
    planes = [
        [r * cols + s * half + i for r in range(rows) for s in range(2)] for i in range(half)
    ]
    pivot_strip = spread(strips[last], 2 * rows, ("row", "col"), planes)
    pivot_strip = jnp.stack([pivot_strip[2 * rows - 3], pivot_strip[2 * rows - 1]])

    eye_strip = lax.dynamic_slice_in_dim(identity, place * tall, tall, 0)
    eye_strip = jnp.where(row - (rows - 2) == core, eye_strip, 0.0)
    left = jnp.concatenate([strips[:last], (strips[last] - eye_strip)[None]], 0)
    left = butterfly(left, lax.dynamic_slice_in_dim(row_scales, place * tall, tall, 2))
    crossed = send(left[:, : tall // 2], crossing)
    piece = jnp.where(side == 1, left[:, tall // 2 :], crossed)
    sent = jnp.concatenate([pivot_strip.reshape(2 * tall, block), piece.reshape(-1, block)], 0)
    pivot_near = spread(sent, ring, "col", rings)
    pivot_far = flip(pivot_near, 1)
    left_across = flip(pivot_near[:, 2 * tall :], span_one)

    cleared = jnp.where(pivot_col, jnp.where(diagonal, identity, 0.0), tail) * col_scales[0]
    tail_one = joined(top_one, cleared, flip(cleared, span_one)) * root_half
    tail_one = tail_one * col_scales[1]
    partner = after(flip(tail_one, span_two), pivot_strip, piece)
    tail_moved = joined(top_two, tail_one, partner) * root_half

    def begun(value, earlier, later):
        value = jnp.where(pivot_col, 0.0, value) * col_scales[0]
        partner = after(flip(value, span_one), *earlier)
        value = joined(top_one, value, partner) * root_half * col_scales[1]
        return value, flip(after(value, *later), span_two)

    lead, lead_far = begun(state[:1], (), ())
    rest, rest_far = begun(state[1:last], (pivot_strip,), (pivot_near,))

    def row_fan(step):
        pairs = [(i, (i + 2 * step) % rows) for i in (rows - 2, rows - 1)]
        return send(tail_moved, pairs, "row")

    near = row_fan(1) + row_fan(2) + row_fan(3)
    near = jnp.where(row >= rows - 2, tail_moved, near)
    far = send(near, [(i, i ^ 1) for i in range(rows)], "row")
    odd_row = row % 2 == 1
    pivot_rows = jnp.stack([jnp.where(odd_row, far, near), jnp.where(odd_row, near, far)])

    matrix = jax.ShapeDtypeStruct((block, block), jnp.float32)
    buffer = pltpu.VMEM((block, block), jnp.float32)
    work = 2 * block**3
    first, below, over, schur = call(
        first_kernel, [matrix] * 4, [buffer] * 2, 160 * work, smem, pivot_near, pivot_far
    )
    left_other = flip(after(left_across, first), 1)
    right = call(
        second_kernel,
        jax.ShapeDtypeStruct((2, block, block), jnp.float32),
        [buffer] * 3,
        160 * work,
        schur,
        first,
        below,
        over,
        pivot_rows,
    )
    lead = joined(top_two, lead, after(lead_far, right)) * root_half
    rest = joined(top_two, rest, after(rest_far, right)) * root_half
    moved = butterfly(jnp.concatenate([lead, rest, tail_moved[None]], 0), row_scales)
    result = call(
        last_kernel,
        jax.ShapeDtypeStruct((blocks * block * block // 128, 128), jnp.float32),
        [],
        6 * 8 * work,
        smem,
        moved,
        pivot_near,
        left_across,
        pivot_far,
        left_other,
        right,
    )
    return result.reshape(inverse_state.shape)


def solution(mesh):
    placed = (P(None, "row", None, "col"), P(None, None, "row"), P(None, None, "col"))

    return jax.shard_map(
        per_device,
        mesh=mesh,
        in_specs=placed,
        out_specs=P(None, "row", None, "col"),
        check_vma=False,
    )
```

```python
import jax
import jax.numpy as jnp
from jax import lax
from jax.experimental import pallas as pl
from jax.experimental.pallas import tpu as pltpu
from jax.sharding import PartitionSpec as P


LIMIT = 64
WARM = 8
root_half = 0.7071067811865476
HIGHEST = lax.Precision.HIGHEST


def seed_values(seeds):
    return (2.0 * seeds.astype(jnp.float32) - 31.0) / 16.0


def halves_level(parts, scales, groups):
    count = parts.shape[0]
    half = count // (2 * groups)
    shaped = parts.reshape((groups, 2, half) + parts.shape[1:])
    factor = scales.reshape((groups, 2, half) + scales.shape[1:])
    upper = factor[:, 0] * shaped[:, 0]
    lower = factor[:, 1] * shaped[:, 1]
    return (jnp.stack([upper + lower, upper - lower], axis=1) * root_half).reshape(parts.shape)


def butterfly(parts, scales):
    return halves_level(halves_level(parts, scales[0], 1), scales[1], 2)


def kdot(a, b, dims=(((1,), (0,)), ((), ())), precision=HIGHEST):
    return lax.dot_general(a, b, dims, precision=precision, preferred_element_type=jnp.float32)


def invert_into(p_ref, x_ref, e_ref):
    size = p_ref.shape[0]
    scale = 1.0 / jnp.max(jnp.abs(p_ref[...]))
    p_ref[...] = p_ref[...] * scale

    def start(precision):
        gram = kdot(p_ref[...], p_ref[...], (((1,), (1,)), ((), ())), precision)
        factor = 1.9 / jnp.max(jnp.sum(jnp.abs(gram), axis=0, keepdims=True))
        x_ref[...] = p_ref[...].T * factor

    def residual(precision):
        row = lax.broadcasted_iota(jnp.int32, (size, size), 0)
        column = lax.broadcasted_iota(jnp.int32, (size, size), 1)
        product = kdot(p_ref[...], x_ref[...], precision=precision)
        e_ref[...] = jnp.where(row == column, 1.0, 0.0) - product

    def advance(precision):
        x_ref[...] += kdot(x_ref[...], e_ref[...], precision=precision)

    def exact_error():
        residual(HIGHEST)
        e = e_ref[...]
        return jnp.sum(e * e)

    start(lax.Precision.DEFAULT)

    @pl.loop(0, WARM)
    def _(_):
        residual(lax.Precision.DEFAULT)
        advance(lax.Precision.DEFAULT)

    error = exact_error()
    failed = jnp.logical_not(error < 0.5)

    @pl.when(failed)
    def _():
        start(HIGHEST)
        residual(HIGHEST)

    def unfinished(carry):
        count, error = carry
        return (count < LIMIT) & jnp.logical_not(error < 1e-7)

    def again(carry):
        advance(HIGHEST)
        return carry[0] + 1, exact_error()

    lax.while_loop(unfinished, again, (0, jnp.where(failed, 1.0, error)))
    advance(HIGHEST)
    x_ref[...] = x_ref[...] * scale


def first_kernel(odd_ref, near_ref, far_ref, first_ref, left_ref, right_ref, schur_ref, p_ref, e_ref):
    odd = odd_ref[0] == 1
    tall = p_ref.shape[0] // near_ref.shape[0]

    def part(i, j):
        at = pl.ds(i * tall, tall)
        near, far = near_ref[:, at], far_ref[:, at]
        return jnp.where(odd == (j == 1), near, far).reshape(p_ref.shape)

    p_ref[...] = part(0, 0)
    invert_into(p_ref, first_ref, e_ref)
    left_ref[...] = kdot(part(1, 0), first_ref[...])
    p_ref[...] = part(0, 1)
    right_ref[...] = kdot(first_ref[...], p_ref[...])
    schur_ref[...] = part(1, 1) - kdot(left_ref[...], p_ref[...])


def second_kernel(schur_ref, first_ref, left_ref, right_ref, rows_ref, out_ref, p_ref, x_ref, e_ref):
    p_ref[...] = schur_ref[...]
    invert_into(p_ref, x_ref, e_ref)
    e_ref[...] = rows_ref[1] - kdot(left_ref[...], rows_ref[0])
    out_ref[1] = kdot(x_ref[...], e_ref[...])
    out_ref[0] = kdot(first_ref[...], rows_ref[0]) - kdot(right_ref[...], out_ref[1])


def last_kernel(place_ref, base_ref, own_ref, across_ref, twin_ref, other_ref, rows_ref, out_ref):
    odd, lower = place_ref[0] == 1, place_ref[1] == 1
    blocks, size = base_ref.shape[:2]
    parts = size // 128
    strip = size // (2 * own_ref.shape[0])
    skip = own_ref.shape[1] - blocks * strip

    def joined(one_ref, two_ref, a):
        one = one_ref[:, skip + a * strip : skip + (a + 1) * strip]
        two = two_ref[:, a * strip : (a + 1) * strip]
        both = jnp.stack([jnp.where(lower, two, one), jnp.where(lower, one, two)], axis=1)
        return both.reshape(size, size)

    for a in range(blocks):
        same, swapped = joined(own_ref, across_ref, a), joined(twin_ref, other_ref, a)
        update = kdot(jnp.where(odd, swapped, same), rows_ref[0])
        update += kdot(jnp.where(odd, same, swapped), rows_ref[1])
        value = base_ref[a] - update
        for lane in range(parts):
            at = pl.ds(a * size * parts + lane, size, stride=parts)
            out_ref[at, :] = value[:, lane * 128 : (lane + 1) * 128]


def call(kernel, out_shape, scratch, flops, *args):
    smem = [pl.BlockSpec(memory_space=pltpu.SMEM)] if args[0].dtype == jnp.int32 else []
    rest = len(args) - len(smem)
    return pl.pallas_call(
        kernel,
        out_shape=out_shape,
        in_specs=smem + [pl.BlockSpec(memory_space=pltpu.VMEM)] * rest,
        out_specs=jax.tree.map(lambda _: pl.BlockSpec(memory_space=pltpu.VMEM), out_shape),
        scratch_shapes=scratch,
        cost_estimate=pl.CostEstimate(flops=flops, bytes_accessed=1 << 20, transcendentals=0),
    )(*args)


def after(value, *earlier):
    return lax.optimization_barrier((value, *earlier))[0]


def per_device(inverse_state, row_seeds, col_seeds):
    blocks, block = inverse_state.shape[:2]
    rows, cols = lax.axis_size("row"), lax.axis_size("col")
    row, col = lax.axis_index("row"), lax.axis_index("col")
    half, ring, last = cols // 2, cols // 4, blocks - 1
    side, place, core = col // half, col % half // 2, col % 2
    rings = [
        [s * half + p * 2 + c for p in range(ring)] for s in range(2) for c in range(2)
    ]
    state = inverse_state.reshape(blocks, block, block)
    identity = jnp.eye(block, dtype=jnp.float32)
    pivot_col = col >= cols - 2
    diagonal = (col - cols == row - rows) & pivot_col
    row_scales = seed_values(row_seeds)[..., None]
    col_scales = seed_values(col_seeds).reshape(2, 1, block)
    smem = jnp.stack([core, side]).astype(jnp.int32)

    def send(value, pairs, axis="col"):
        return lax.ppermute(value, axis, pairs)

    def flip(value, bit):
        return send(value, [(i, i ^ bit) for i in range(cols)])

    def exchange(parts, axis, groups=None):
        return lax.all_to_all(parts, axis, 0, 0, axis_index_groups=groups)

    def spread(part, count, axis, groups=None):
        return exchange(jnp.broadcast_to(part, (count,) + part.shape), axis, groups)

    def joined(top, own, partner):
        return jnp.where(top, own + partner, partner - own)

    span_one, span_two = half, half // 2
    top_one, top_two = col // span_one % 2 == 0, col // span_two % 2 == 0

    tail = state[last]
    tall = block // ring
    strips = state.reshape(blocks, ring, tall, block).transpose(1, 0, 2, 3)
    strips = exchange(strips, "col", rings)[ring - 1]
    crossing = [(i + half, i) for i in range(half)]
    planes = [
        [r * cols + s * half + i for r in range(rows) for s in range(2)] for i in range(half)
    ]
    pivot_strip = spread(strips[last], 2 * rows, ("row", "col"), planes)
    pivot_strip = jnp.stack([pivot_strip[2 * rows - 3], pivot_strip[2 * rows - 1]])

    eye_strip = lax.dynamic_slice_in_dim(identity, place * tall, tall, 0)
    eye_strip = jnp.where(row - (rows - 2) == core, eye_strip, 0.0)
    left = jnp.concatenate([strips[:last], (strips[last] - eye_strip)[None]], 0)
    left = butterfly(left, lax.dynamic_slice_in_dim(row_scales, place * tall, tall, 2))
    crossed = send(left[:, : tall // 2], crossing)
    piece = jnp.where(side == 1, left[:, tall // 2 :], crossed)
    sent = jnp.concatenate([pivot_strip.reshape(2 * tall, block), piece.reshape(-1, block)], 0)
    pivot_near = spread(sent, ring, "col", rings)
    pivot_far = flip(pivot_near[:, : 2 * tall], 1)
    left_own = pivot_near[:, 2 * tall :]
    left_across = flip(left_own, span_one)
    left_twin = flip(left_own, 1)

    cleared = jnp.where(pivot_col, jnp.where(diagonal, identity, 0.0), tail) * col_scales[0]
    tail_one = joined(top_one, cleared, flip(cleared, span_one)) * root_half
    tail_one = tail_one * col_scales[1]
    partner = after(flip(tail_one, span_two), pivot_strip, piece)
    tail_moved = joined(top_two, tail_one, partner) * root_half

    def begun(value, earlier, later):
        value = jnp.where(pivot_col, 0.0, value) * col_scales[0]
        partner = after(flip(value, span_one), *earlier)
        value = joined(top_one, value, partner) * root_half * col_scales[1]
        return value, flip(after(value, *later), span_two)

    lead, lead_far = begun(state[:1], (), ())
    rest, rest_far = begun(state[1:last], (pivot_strip,), (pivot_near,))

    def row_fan(step):
        pairs = [(i, (i + 2 * step) % rows) for i in (rows - 2, rows - 1)]
        return send(tail_moved, pairs, "row")

    near = row_fan(1) + row_fan(2) + row_fan(3)
    near = jnp.where(row >= rows - 2, tail_moved, near)
    far = send(near, [(i, i ^ 1) for i in range(rows)], "row")
    odd_row = row % 2 == 1
    pivot_rows = jnp.stack([jnp.where(odd_row, far, near), jnp.where(odd_row, near, far)])

    matrix = jax.ShapeDtypeStruct((block, block), jnp.float32)
    buffer = pltpu.VMEM((block, block), jnp.float32)
    work = 2 * block**3
    first, below, over, schur = call(
        first_kernel, [matrix] * 4, [buffer] * 2, 160 * work, smem, pivot_near, pivot_far
    )
    left_other = flip(after(left_across, first), 1)
    right = call(
        second_kernel,
        jax.ShapeDtypeStruct((2, block, block), jnp.float32),
        [buffer] * 3,
        160 * work,
        schur,
        first,
        below,
        over,
        pivot_rows,
    )
    lead = joined(top_two, lead, after(lead_far, right)) * root_half
    rest = joined(top_two, rest, after(rest_far, right)) * root_half
    moved = butterfly(jnp.concatenate([lead, rest, tail_moved[None]], 0), row_scales)
    result = call(
        last_kernel,
        jax.ShapeDtypeStruct((blocks * block * block // 128, 128), jnp.float32),
        [],
        6 * 8 * work,
        smem,
        moved,
        left_own,
        left_across,
        left_twin,
        left_other,
        right,
    )
    return result.reshape(inverse_state.shape)


def solution(mesh):
    placed = (P(None, "row", None, "col"), P(None, None, "row"), P(None, None, "col"))

    return jax.shard_map(
        per_device,
        mesh=mesh,
        in_specs=placed,
        out_specs=P(None, "row", None, "col"),
        check_vma=False,
    )
```
